16 devices in a mesh: rep: 2 (over y, z), dp: 8 (over x, core).
Axes of the slice: x: 4, y: 2, z: 1, core: 2. Of those that a mesh axis runs over, the one named last changes fastest.
The devices are a block of a 4x4x8 slice.
Arguments:
- hidden: bfloat16 [1024, 2560], P(('rep', 'dp')), parts along dimension 0
- ckv_cache: bfloat16 [1024, 1024, 256], P(('rep', 'dp')), parts along dimension 0
- kpe_cache: bfloat16 [1024, 1024, 32], P(('rep', 'dp')), parts along dimension 0
- cache_len: int32 [1024], P(('rep', 'dp')), parts along dimension 0
- rope_cos: float32 [1024, 16], P(('rep', 'dp')), parts along dimension 0
- rope_sin: float32 [1024, 16], P(('rep', 'dp')), parts along dimension 0
- norm_attn: float32 [2560], replicated
- w_dq: bfloat16 [2560, 768], replicated
- norm_q: float32 [768], replicated
- w_uq: bfloat16 [768, 40, 96], replicated
- w_dkv: bfloat16 [2560, 288], replicated
- norm_kv: float32 [256], replicated
- w_uk: bfloat16 [256, 40, 64], replicated
- w_uv: bfloat16 [256, 40, 64], replicated
- w_out: bfloat16 [40, 64, 2560], replicated
- norm_mlp: float32 [2560], replicated
- w_gate: bfloat16 [2560, 6400], P(None, 'dp')
- w_up: bfloat16 [2560, 6400], P(None, 'dp')
- w_down: bfloat16 [6400, 2560], P('dp')
Outputs:
- output 1: bfloat16 [1024, 2560], P(('rep', 'dp')), parts along dimension 0
- output 2: bfloat16 [1024, 256], P(('rep', 'dp')), parts along dimension 0
- output 3: bfloat16 [1024, 32], P(('rep', 'dp')), parts along dimension 0
There are 2 independent parts. The reference program is written for one: setup_inputs(seed, part) draws one part's arguments, and reference() takes and returns one part's arrays. A program takes and returns all parts, laid end to end along the dimension named above; an argument that names none is the same for every part.
All inputs are finite; a program needn't handle non-finite values.
Results may differ from the reference program's by a relative error of at most 0.010691.
Values are sent between devices in bfloat16 or wider.
A program may use at most 768 MiB of HBM per device.

```python
import math
import jax
import jax.numpy as jnp
from jax import lax

BATCH = 512
SEQ_LEN = 1024
D_MODEL = 2560
HEADS = 40
Q_LORA = 768
KV_LORA = 256
NOPE_DIM = 64
ROPE_DIM = 32
V_HEAD = 64
FF_DIM = 6400

EPSILON = 1e-6
MSCALE = 0.1 * math.log(40.0) + 1.0
SCORE_SCALE = MSCALE * MSCALE / math.sqrt(NOPE_DIM + ROPE_DIM)


def weight_draw(rand_key, arr_shape, fan_in):
    return (jax.random.normal(rand_key, arr_shape, jnp.float32) * fan_in ** -0.5).astype(jnp.bfloat16)


def gain_draw(rand_key, vec_size):
    return 1.0 + 0.3 * jax.random.normal(rand_key, (vec_size,), jnp.float32)


def setup_inputs(seed: int = 0, part: int = 0) -> dict:
    base_key = jax.random.key(seed)
    shared_keys = jax.random.split(base_key, 16)
    part_keys = jax.random.split(jax.random.fold_in(base_key, part), 8)
    half_rope = ROPE_DIM // 2
    hidden = jax.random.normal(part_keys[0], (BATCH, D_MODEL), jnp.float32).astype(jnp.bfloat16)
    centre = jax.random.normal(part_keys[1], (BATCH, 1, KV_LORA), jnp.float32)
    spread = jax.random.normal(part_keys[2], (BATCH, SEQ_LEN, KV_LORA), jnp.float32)
    ckv_cache = (0.6 * centre + 0.8 * spread).astype(jnp.bfloat16)
    kpe_cache = jax.random.normal(part_keys[3], (BATCH, SEQ_LEN, ROPE_DIM), jnp.float32).astype(jnp.bfloat16)
    base_len = jax.random.randint(part_keys[4], (BATCH,), 1, SEQ_LEN)
    pick_rows = jax.random.randint(part_keys[5], (2,), 0, BATCH)
    long_row = pick_rows[0]
    short_row = (long_row + 1 + pick_rows[1] % (BATCH - 1)) % BATCH
    cache_len = base_len.at[long_row].set(SEQ_LEN - 1).at[short_row].set(1)
    inv_freq = 10000.0 ** (-jnp.arange(half_rope, dtype=jnp.float32) / half_rope)
    angles = cache_len.astype(jnp.float32)[:, None] * inv_freq[None, :]
    return dict(
        hidden=hidden,
        ckv_cache=ckv_cache,
        kpe_cache=kpe_cache,
        cache_len=cache_len,
        rope_cos=jnp.cos(angles),
        rope_sin=jnp.sin(angles),
        norm_attn=gain_draw(shared_keys[0], D_MODEL),
        w_dq=weight_draw(shared_keys[1], (D_MODEL, Q_LORA), D_MODEL),
        norm_q=gain_draw(shared_keys[2], Q_LORA),
        w_uq=weight_draw(shared_keys[3], (Q_LORA, HEADS, NOPE_DIM + ROPE_DIM), Q_LORA),
        w_dkv=weight_draw(shared_keys[4], (D_MODEL, KV_LORA + ROPE_DIM), D_MODEL),
        norm_kv=gain_draw(shared_keys[5], KV_LORA),
        w_uk=weight_draw(shared_keys[6], (KV_LORA, HEADS, NOPE_DIM), NOPE_DIM),
        w_uv=weight_draw(shared_keys[7], (KV_LORA, HEADS, V_HEAD), KV_LORA),
        w_out=weight_draw(shared_keys[8], (HEADS, V_HEAD, D_MODEL), HEADS * V_HEAD),
        norm_mlp=gain_draw(shared_keys[9], D_MODEL),
        w_gate=weight_draw(shared_keys[10], (D_MODEL, FF_DIM), D_MODEL),
        w_up=weight_draw(shared_keys[11], (D_MODEL, FF_DIM), D_MODEL),
        w_down=weight_draw(shared_keys[12], (FF_DIM, D_MODEL), FF_DIM),
    )


def rms_norm(values_in, gain_vec):
    floats = values_in.astype(jnp.float32)
    mean_sq = jnp.mean(floats * floats, axis=-1, keepdims=True)
    return floats * lax.rsqrt(mean_sq + EPSILON) * gain_vec.astype(jnp.float32)


def apply_rope(values_in, cos_t, sin_t):
    half_dim = values_in.shape[-1] // 2
    low_half = values_in[..., :half_dim]
    high_half = values_in[..., half_dim:]
    return jnp.concatenate([low_half * cos_t - high_half * sin_t, high_half * cos_t + low_half * sin_t], axis=-1)


def one_request(operands):
    q_abs_row, q_pe_row, ckv_row, kpe_row, len_row, ckv_new_row, kpe_new_row = operands
    ckv_float = ckv_row.astype(jnp.float32)
    scores = (jnp.einsum('hl,tl->ht', q_abs_row.astype(jnp.float32), ckv_float)
              + jnp.einsum('hr,tr->ht', q_pe_row.astype(jnp.float32), kpe_row.astype(jnp.float32))) * SCORE_SCALE
    scores = jnp.where(jnp.arange(SEQ_LEN)[None, :] < len_row, scores, -jnp.inf)
    score_new = (jnp.dot(q_abs_row.astype(jnp.float32), ckv_new_row.astype(jnp.float32))
                 + jnp.dot(q_pe_row.astype(jnp.float32), kpe_new_row.astype(jnp.float32))) * SCORE_SCALE
    row_max = jnp.maximum(jnp.max(scores, axis=1), score_new)
    exp_cache = jnp.exp(scores - row_max[:, None])
    exp_new = jnp.exp(score_new - row_max)
    norm_sum = jnp.sum(exp_cache, axis=1) + exp_new
    weighted = (jnp.einsum('ht,tl->hl', exp_cache.astype(jnp.bfloat16).astype(jnp.float32), ckv_float)
                + exp_new.astype(jnp.bfloat16).astype(jnp.float32)[:, None] * ckv_new_row.astype(jnp.float32)[None, :])
    return (weighted / norm_sum[:, None]).astype(jnp.bfloat16)


def reference(hidden, ckv_cache, kpe_cache, cache_len, rope_cos, rope_sin, norm_attn, w_dq, norm_q, w_uq, w_dkv, norm_kv, w_uk, w_uv, w_out, norm_mlp, w_gate, w_up, w_down):
    normed = rms_norm(hidden, norm_attn).astype(jnp.bfloat16)
    q_latent = rms_norm(jnp.dot(normed, w_dq, preferred_element_type=jnp.float32), norm_q).astype(jnp.bfloat16)
    q_full = jnp.einsum('bl,lhe->bhe', q_latent.astype(jnp.float32), w_uq.astype(jnp.float32))
    q_nope = q_full[..., :NOPE_DIM].astype(jnp.bfloat16)
    q_pe = apply_rope(q_full[..., NOPE_DIM:], rope_cos[:, None, :], rope_sin[:, None, :]).astype(jnp.bfloat16)
    kv_full = jnp.dot(normed, w_dkv, preferred_element_type=jnp.float32)
    ckv_new = rms_norm(kv_full[:, :KV_LORA], norm_kv).astype(jnp.bfloat16)
    kpe_new = apply_rope(kv_full[:, KV_LORA:], rope_cos, rope_sin).astype(jnp.bfloat16)
    q_abs = jnp.einsum('bhn,lhn->bhl', q_nope.astype(jnp.float32), w_uk.astype(jnp.float32)).astype(jnp.bfloat16)
    lat_out = lax.map(one_request, (q_abs, q_pe, ckv_cache, kpe_cache, cache_len, ckv_new, kpe_new))
    head_out = jnp.einsum('bhl,lhv->bhv', lat_out.astype(jnp.float32), w_uv.astype(jnp.float32)).astype(jnp.bfloat16)
    attn_out = jnp.einsum('bhv,hvd->bd', head_out.astype(jnp.float32), w_out.astype(jnp.float32))
    residual = (hidden.astype(jnp.float32) + attn_out).astype(jnp.bfloat16)
    mlp_in = rms_norm(residual, norm_mlp).astype(jnp.bfloat16)
    gate_val = jnp.dot(mlp_in, w_gate, preferred_element_type=jnp.float32)
    up_val = jnp.dot(mlp_in, w_up, preferred_element_type=jnp.float32)
    act_val = (jax.nn.silu(gate_val) * up_val).astype(jnp.bfloat16)
    mlp_out = jnp.dot(act_val, w_down, preferred_element_type=jnp.float32)
    out_hidden = (residual.astype(jnp.float32) + mlp_out).astype(jnp.bfloat16)
    return (out_hidden, ckv_new, kpe_new)
```

```python
import functools
import math

import jax
import jax.numpy as jnp
from jax import lax
from jax.experimental import pallas as pl
from jax.experimental.pallas import tpu as pltpu
from jax.sharding import PartitionSpec as P

EPSILON = 1e-6
MSCALE = 0.1 * math.log(40.0) + 1.0
F32 = jnp.float32
BF16 = jnp.bfloat16
NT = (((1,), (1,)), ((), ()))
VMEM_LIMIT = 64 * 1024 * 1024 - 65536


def dot(a, b):
    return jnp.dot(a, b, preferred_element_type=F32)


def dot_nt(a, b):
    return lax.dot_general(a, b, NT, preferred_element_type=F32)


def normed(v, gain):
    return v * lax.rsqrt(jnp.mean(v * v, axis=-1, keepdims=True) + EPSILON) * gain


def attention_kernel(dims, len_ref, x_ref, g1_ref, gq_ref, gkv_ref, g2_ref, cos_ref, sin_ref,
                     wdq_hbm, wdkv_hbm, wuq_hbm, wuk_hbm, wuv_hbm, wout_hbm, ckv_hbm, kpe_hbm,
                     r_ref, u_ref, cnew_ref, knew_ref,
                     ql_s, qr_s, cn_s, kn_s, o_s, tr_s,
                     wdq, wdkv, wuq, wuk, wuv, wout, ckv_b, kpe_b, wsem, csem):
    heads, nope, rope, qk, lat, per, slots = dims
    rows = x_ref.shape[0]
    seq = ckv_hbm.shape[1]
    half = rope // 2
    steps = rows // per
    scale = MSCALE * MSCALE / math.sqrt(qk)

    def wcopy(src, dst, i):
        return pltpu.make_async_copy(src, dst, wsem.at[i])

    def ccopy(step, slot):
        at = pl.ds(step * per, per)
        return (pltpu.make_async_copy(ckv_hbm.at[at], ckv_b.at[slot], csem.at[slot, 0]),
                pltpu.make_async_copy(kpe_hbm.at[at], kpe_b.at[slot], csem.at[slot, 1]))

    c_dq = wcopy(wdq_hbm, wdq, 0)
    c_dkv = wcopy(wdkv_hbm, wdkv, 1)
    c_uk = wcopy(wuk_hbm, wuk, 2)
    c_uq = wcopy(wuq_hbm, wuq, 3)
    c_uv = wcopy(wuv_hbm, wuv, 4)
    c_out = wcopy(wout_hbm, wout, 5)
    for c in (c_dq, c_dkv, c_uk, c_uq):
        c.start()
    for s in range(slots):
        for c in ccopy(s, s):
            c.start()
    c_uv.start()
    c_out.start()

    tr_s[...] = jnp.zeros_like(tr_s)
    cos_t, sin_t = cos_ref[...], sin_ref[...]
    tr_s[0:half, 0:rows] = cos_t
    tr_s[half:rope, 0:rows] = cos_t
    tr_s[rope:rope + half, 0:rows] = -sin_t
    tr_s[rope + half:2 * rope, 0:rows] = sin_t
    table = tr_s[...].T[0:rows]
    cos2, sin2 = table[:, 0:rope], pltpu.roll(table, 128 - rope, axis=1)[:, 0:rope]
    group = 256 // rope
    cos_g = jnp.concatenate([cos2] * group, axis=1)
    sin_g = jnp.concatenate([sin2] * group, axis=1)

    a = normed(x_ref[...].astype(F32), g1_ref[...]).astype(BF16)
    c_dq.wait()
    cq = normed(dot(a, wdq[...]), gq_ref[...]).astype(BF16)
    c_dkv.wait()
    cn = normed(dot_nt(a, wdkv[0:lat]), gkv_ref[...]).astype(BF16)
    cnew_ref[...] = cn
    cn_s[...] = cn.astype(F32)
    kp = dot_nt(a, wdkv[lat:lat + rope])
    ks = dot_nt(a, jnp.concatenate([wdkv[lat + half:lat + rope], wdkv[lat:lat + half]], axis=0))
    kn = (kp * cos2 + ks * sin2).astype(BF16).astype(F32)
    kn_s[...] = kn
    tr_s[...] = jnp.zeros_like(tr_s)
    tr_s[0:rows, 0:rope] = kn
    knew_ref[...] = tr_s[...].T[0:rope, 0:rows].astype(BF16)

    c_uk.wait()
    c_uq.wait()
    lane = lax.broadcasted_iota(jnp.int32, (rows, 2 * nope), 1)

    def project(g, carry):
        base = g * (group * qk)
        for quad in range(group // 4):
            wn = jnp.concatenate(
                [wuq[pl.ds(pl.multiple_of(base + (quad * 4 + j) * qk, 32), nope), :] for j in range(4)], axis=0)
            q4 = dot_nt(cq, wn)
            for pair in range(2):
                qp = q4[:, pair * 2 * nope:(pair + 1) * 2 * nope]
                both = jnp.concatenate([jnp.where(lane < nope, qp, 0.0), jnp.where(lane >= nope, qp, 0.0)], axis=0)
                first = g * group + quad * 4 + pair * 2
                wk = wuk[pl.ds(pl.multiple_of(first * nope, 128), 2 * nope), :]
                ql = dot(both.astype(BF16), wk)
                ql = ql.astype(BF16).astype(F32)
                for i in range(lat // 128):
                    ql_s[i, pl.ds(pl.multiple_of(first * rows, 128), 2 * rows), :] = ql[:, i * 128:(i + 1) * 128]
        lows = [wuq[pl.ds(pl.multiple_of(base + j * qk + nope, 16), half), :] for j in range(group)]
        highs = [wuq[pl.ds(pl.multiple_of(base + j * qk + nope + half, 16), half), :] for j in range(group)]
        wp = jnp.concatenate([w for j in range(group) for w in (lows[j], highs[j])], axis=0)
        ws = jnp.concatenate([w for j in range(group) for w in (highs[j], lows[j])], axis=0)
        qr = (dot_nt(cq, wp) * cos_g + dot_nt(cq, ws) * sin_g).astype(BF16).astype(F32)
        for j in range(group):
            part = qr[:, 128 * (j * rope // 128):128 * (j * rope // 128) + 128]
            shift = (128 - (j * rope) % 128) % 128
            if shift:
                part = pltpu.roll(part, shift, axis=1)
            qr_s[pl.ds(pl.multiple_of((g * group + j) * rows, 64), rows), :] = part
        return carry

    lax.fori_loop(0, heads // group, project, 0)

    position = lax.broadcasted_iota(jnp.int32, (heads, seq), 1)

    def attend(step, carry):
        slot = lax.rem(step, slots)
        for c in ccopy(step, slot):
            c.wait()
        for j in range(per):
            b = step * per + j
            ql = jnp.concatenate([ql_s[i, pl.ds(b, heads, stride=rows), :] for i in range(lat // 128)], axis=1)
            qr = qr_s[pl.ds(b, heads, stride=rows), :][:, 0:rope]
            ck = ckv_b[slot, j]
            s = (dot_nt(ql.astype(BF16), ck) + dot(qr.astype(BF16), kpe_b[slot, j])) * scale
            s = jnp.where(position < len_ref[b], s, -jnp.inf)
            cn_b = cn_s[pl.ds(b, 1), :]
            kn_b = kn_s[pl.ds(b, 1), :]
            s_new = (jnp.sum(ql * cn_b, axis=1, keepdims=True) + jnp.sum(qr * kn_b, axis=1, keepdims=True)) * scale
            m = jnp.maximum(jnp.max(s, axis=1, keepdims=True), s_new)
            e = jnp.exp(s - m)
            e_new = jnp.exp(s_new - m)
            total = jnp.sum(e, axis=1, keepdims=True) + e_new
            acc = dot(e.astype(BF16), ck) + e_new.astype(BF16).astype(F32) * cn_b
            out = (acc / total).astype(BF16).astype(F32)
            for i in range(lat // 128):
                ql_s[i, pl.ds(b, heads, stride=rows), :] = out[:, i * 128:(i + 1) * 128]

        @pl.when(step + slots < steps)
        def _():
            for c in ccopy(step + slots, slot):
                c.start()

        return carry

    lax.fori_loop(0, steps, attend, 0)

    c_uv.wait()
    quad_lane = lax.broadcasted_iota(jnp.int32, (rows, 4 * nope), 1) // nope

    def head_out(g, carry):
        at = pl.ds(pl.multiple_of(g * 4 * rows, 256), 4 * rows)
        lat_out = jnp.concatenate([ql_s[i, at, :] for i in range(lat // 128)], axis=1).astype(BF16)
        full = dot_nt(lat_out, wuv[pl.ds(pl.multiple_of(g * 4 * nope, 256), 4 * nope), :])
        o = full[0:rows]
        for j in range(1, 4):
            o = jnp.where(quad_lane == j, full[j * rows:(j + 1) * rows], o)
        o_s[g] = o.astype(BF16)
        return carry

    lax.fori_loop(0, heads // 4, head_out, 0)

    c_out.wait()
    o_all = jnp.concatenate([o_s[g] for g in range(heads // 4)], axis=1)
    width = 512
    sq = jnp.zeros((rows, 1), F32)
    for n in range(wout.shape[1] // width):
        at = slice(n * width, (n + 1) * width)
        res = (x_ref[:, at].astype(F32) + dot(o_all, wout[:, at])).astype(BF16)
        r_ref[:, at] = res
    u_ref[...] = normed(r_ref[...].astype(F32), g2_ref[...]).astype(BF16)


def attention_rows(hidden, ckv_cache, kpe_cache, cache_len, rope_cos, rope_sin, norm_attn, w_dq, norm_q, w_uq, w_dkv, norm_kv, w_uk, w_uv, w_out, norm_mlp):
    rows, width = hidden.shape
    q_lora, heads, qk = w_uq.shape
    lat, _, nope = w_uk.shape
    rope = kpe_cache.shape[2]
    seq = ckv_cache.shape[1]
    per, slots = 4, 3
    dims = (heads, nope, rope, qk, lat, per, slots)
    vm = pl.BlockSpec(memory_space=pltpu.VMEM)
    hbm = pl.BlockSpec(memory_space=pl.ANY)
    wdkv_t = w_dkv.T
    wuq_t = w_uq.transpose(1, 2, 0).reshape(heads * qk, q_lora)
    wuk_t = w_uk.transpose(1, 2, 0).reshape(heads * nope, lat)
    wuv_t = w_uv.transpose(1, 2, 0).reshape(heads * nope, lat)
    wout2 = w_out.reshape(heads * nope, width)
    r, u, cn, kn_t = pl.pallas_call(
        functools.partial(attention_kernel, dims),
        out_shape=(jax.ShapeDtypeStruct((rows, width), BF16), jax.ShapeDtypeStruct((rows, width), BF16),
                   jax.ShapeDtypeStruct((rows, lat), BF16), jax.ShapeDtypeStruct((rope, rows), BF16)),
        in_specs=[pl.BlockSpec(memory_space=pltpu.SMEM)] + [vm] * 7 + [hbm] * 8,
        out_specs=(vm,) * 4,
        scratch_shapes=[
            pltpu.VMEM((lat // 128, heads * rows, 128), F32),
            pltpu.VMEM((heads * rows, 128), F32),
            pltpu.VMEM((rows, lat), F32),
            pltpu.VMEM((rows, rope), F32),
            pltpu.VMEM((heads // 4, rows, 4 * nope), BF16),
            pltpu.VMEM((128, 128), F32),
            pltpu.VMEM(w_dq.shape, BF16),
            pltpu.VMEM(wdkv_t.shape, BF16),
            pltpu.VMEM(wuq_t.shape, BF16),
            pltpu.VMEM(wuk_t.shape, BF16),
            pltpu.VMEM(wuv_t.shape, BF16),
            pltpu.VMEM(wout2.shape, BF16),
            pltpu.VMEM((slots, per, seq, lat), BF16),
            pltpu.VMEM((slots, per, rope, seq), BF16),
            pltpu.SemaphoreType.DMA((6,)),
            pltpu.SemaphoreType.DMA((slots, 2)),
        ],
        compiler_params=pltpu.CompilerParams(vmem_limit_bytes=VMEM_LIMIT),
        name="attention",
    )(cache_len, hidden, norm_attn.reshape(1, -1), norm_q.reshape(1, -1), norm_kv.reshape(1, -1), norm_mlp.reshape(1, -1),
      rope_cos.T, rope_sin.T, w_dq, wdkv_t, wuq_t, wuk_t, wuv_t, wout2, ckv_cache, kpe_cache.transpose(0, 2, 1))
    return r, u, cn, kn_t.T


def solution(mesh):
    row_spec = P(('rep', 'dp'), None)
    cube_spec = P(('rep', 'dp'), None, None)
    full_spec = P()
    in_specs = (row_spec, cube_spec, cube_spec, P(('rep', 'dp')), row_spec, row_spec,
                full_spec, full_spec, full_spec, full_spec, full_spec, full_spec, full_spec, full_spec, full_spec, full_spec,
                P(None, 'dp'), P(None, 'dp'), P('dp', None))

    def local_step(hidden, ckv_cache, kpe_cache, cache_len, rope_cos, rope_sin, norm_attn, w_dq, norm_q, w_uq, w_dkv, norm_kv, w_uk, w_uv, w_out, norm_mlp, w_gate, w_up, w_down):
        residual, mlp_in, ckv_new, kpe_new = attention_rows(
            hidden, ckv_cache, kpe_cache, cache_len, rope_cos, rope_sin, norm_attn, w_dq, norm_q, w_uq, w_dkv, norm_kv, w_uk, w_uv, w_out, norm_mlp)
        group_in = lax.all_gather(mlp_in, 'dp', axis=0, tiled=True)
        gate_val = jnp.dot(group_in, w_gate, preferred_element_type=jnp.float32)
        up_val = jnp.dot(group_in, w_up, preferred_element_type=jnp.float32)
        act_val = (jax.nn.silu(gate_val) * up_val).astype(jnp.bfloat16)
        partial_sum = jnp.dot(act_val, w_down, preferred_element_type=jnp.float32)
        mlp_rows = lax.psum_scatter(partial_sum, 'dp', scatter_dimension=0, tiled=True)
        out_hidden = (residual.astype(jnp.float32) + mlp_rows).astype(jnp.bfloat16)
        return out_hidden, ckv_new, kpe_new

    return jax.shard_map(local_step, mesh=mesh, in_specs=in_specs, out_specs=(row_spec, row_spec, row_spec), check_vma=False)
```

```python
import functools
import math

import jax
import jax.numpy as jnp
from jax import lax
from jax.experimental import pallas as pl
from jax.experimental.pallas import tpu as pltpu
from jax.sharding import PartitionSpec as P

EPSILON = 1e-6
MSCALE = 0.1 * math.log(40.0) + 1.0
F32 = jnp.float32
BF16 = jnp.bfloat16
NT = (((1,), (1,)), ((), ()))
VMEM_LIMIT = 64 * 1024 * 1024 - 65536


def dot(a, b):
    return jnp.dot(a, b, preferred_element_type=F32)


def dot_nt(a, b):
    return lax.dot_general(a, b, NT, preferred_element_type=F32)


def normed(v, gain):
    return v * lax.rsqrt(jnp.mean(v * v, axis=-1, keepdims=True) + EPSILON) * gain


class Copies:
    def __init__(self, copies):
        self.copies = copies

    def start(self):
        for c in self.copies:
            c.start()

    def wait(self):
        for c in self.copies:
            c.wait()


def wide(ref, rows=slice(None)):
    return jnp.concatenate([ref[c, rows, :] for c in range(ref.shape[0])], axis=1)


def attention_kernel(dims, len_ref, x_ref, g1_ref, gq_ref, gkv_ref, g2_ref, cos_ref, sin_ref,
                     wdq_hbm, wdkv_hbm, wuq_hbm, wuk_hbm, wuv_hbm, wout_hbm, ckv_hbm, kpe_hbm,
                     r_ref, u_ref, cnew_ref, knew_ref,
                     ql_s, qr_s, cn_s, kn_s, o_s, tr_s,
                     wdq, wdkv, wuq, wuk, wuv, wout, ckv_b, kpe_b, wsem, csem):
    heads, nope, rope, qk, lat, per, slots = dims
    rows = x_ref.shape[0]
    seq = ckv_hbm.shape[1]
    half = rope // 2
    steps = rows // per
    scale = MSCALE * MSCALE / math.sqrt(qk)

    def wcopy(src, dst, i, rows_at=slice(None)):
        return Copies([pltpu.make_async_copy(src.at[rows_at, pl.ds(c * 128, 128)], dst.at[c, rows_at], wsem.at[i])
                       for c in range(dst.shape[0])])

    def ccopy(step, slot):
        at = pl.ds(step * per, per)
        return [pltpu.make_async_copy(ckv_hbm.at[at, :, pl.ds(c * 128, 128)], ckv_b.at[slot, c], csem.at[slot, c])
                for c in range(lat // 128)] + [
                    pltpu.make_async_copy(kpe_hbm.at[at], kpe_b.at[slot], csem.at[slot, lat // 128])]

    group = 256 // rope
    groups = heads // group
    c_dq = wcopy(wdq_hbm, wdq, 0)
    c_dkv = wcopy(wdkv_hbm, wdkv, 1)
    c_uk = wcopy(wuk_hbm, wuk, 2)
    c_uv = wcopy(wuv_hbm, wuv, 3)
    c_out = wcopy(wout_hbm, wout, 4)

    def c_uq(g):
        return wcopy(wuq_hbm, wuq, 5 + g, pl.ds(pl.multiple_of(g * group * qk, 256), group * qk))

    for c in (c_dq, c_dkv, c_uk):
        c.start()
    for g in range(groups):
        c_uq(g).start()
    for s in range(slots):
        for c in ccopy(s, s):
            c.start()
    c_uv.start()
    c_out.start()

    tr_s[...] = jnp.zeros_like(tr_s)
    cos_t, sin_t = cos_ref[...], sin_ref[...]
    tr_s[0:half, 0:rows] = cos_t
    tr_s[half:rope, 0:rows] = cos_t
    tr_s[rope:rope + half, 0:rows] = -sin_t
    tr_s[rope + half:2 * rope, 0:rows] = sin_t
    table = tr_s[...].T[0:rows]
    cos2, sin2 = table[:, 0:rope], pltpu.roll(table, 128 - rope, axis=1)[:, 0:rope]
    cos_g = jnp.concatenate([cos2] * group, axis=1)
    sin_g = jnp.concatenate([sin2] * group, axis=1)

    a = normed(x_ref[...].astype(F32), g1_ref[...]).astype(BF16)
    with jax.named_scope("w_dq"):
        c_dq.wait()
    with jax.named_scope("dqkv"):
        cq = normed(dot(a, wide(wdq)), gq_ref[...]).astype(BF16)
        c_dkv.wait()
        cn = normed(dot_nt(a, wide(wdkv, slice(0, lat))), gkv_ref[...]).astype(BF16)
        cnew_ref[...] = cn
        cn_s[...] = cn.astype(F32)
        w_kp = wide(wdkv, slice(lat, lat + rope))
        kp = dot_nt(a, w_kp)
        ks = dot_nt(a, jnp.concatenate([w_kp[half:], w_kp[:half]], axis=0))
        kn = (kp * cos2 + ks * sin2).astype(BF16).astype(F32)
        kn_s[...] = kn
        tr_s[...] = jnp.zeros_like(tr_s)
        tr_s[0:rows, 0:rope] = kn
        knew_ref[...] = tr_s[...].T[0:rope, 0:rows].astype(BF16)

    with jax.named_scope("w_uk"):
        c_uk.wait()
    lane = lax.broadcasted_iota(jnp.int32, (rows, 2 * nope), 1)

    def project(g, carry):
        base = g * (group * qk)
        with jax.named_scope("w_uq"):
            c_uq(g).wait()
        with jax.named_scope("proj"):
            for quad in range(group // 4):
                wn = jnp.concatenate(
                    [wide(wuq, pl.ds(pl.multiple_of(base + (quad * 4 + j) * qk, 32), nope)) for j in range(4)], axis=0)
                q4 = dot_nt(cq, wn)
                for pair in range(2):
                    qp = q4[:, pair * 2 * nope:(pair + 1) * 2 * nope]
                    both = jnp.concatenate([jnp.where(lane < nope, qp, 0.0), jnp.where(lane >= nope, qp, 0.0)], axis=0)
                    first = g * group + quad * 4 + pair * 2
                    wk = wide(wuk, pl.ds(pl.multiple_of(first * nope, 128), 2 * nope))
                    ql = dot(both.astype(BF16), wk)
                    ql = ql.astype(BF16).astype(F32)
                    for i in range(lat // 128):
                        for k in range(2):
                            ql_s.at[i][pl.ds(first + k, rows, stride=heads), :] = ql[k * rows:(k + 1) * rows, i * 128:(i + 1) * 128]
            lows = [wide(wuq, pl.ds(pl.multiple_of(base + j * qk + nope, 16), half)) for j in range(group)]
            highs = [wide(wuq, pl.ds(pl.multiple_of(base + j * qk + nope + half, 16), half)) for j in range(group)]
            wp = jnp.concatenate([w for j in range(group) for w in (lows[j], highs[j])], axis=0)
            ws = jnp.concatenate([w for j in range(group) for w in (highs[j], lows[j])], axis=0)
            qr = (dot_nt(cq, wp) * cos_g + dot_nt(cq, ws) * sin_g).astype(BF16).astype(F32)
            for j in range(group):
                part = qr[:, 128 * (j * rope // 128):128 * (j * rope // 128) + 128]
                shift = (128 - (j * rope) % 128) % 128
                if shift:
                    part = pltpu.roll(part, shift, axis=1)
                qr_s[pl.ds(g * group + j, rows, stride=heads), :] = part
        return carry

    lax.fori_loop(0, heads // group, project, 0)

    position = lax.broadcasted_iota(jnp.int32, (heads, seq), 1)

    def attend(step, carry):
        slot = lax.rem(step, slots)
        with jax.named_scope("cwait"):
            for c in ccopy(step, slot):
                c.wait()
        with jax.named_scope("attn"):
            for j in range(per):
                b = step * per + j
                mine = pl.ds(pl.multiple_of(b * heads, 8), heads)
                ql = jnp.concatenate([ql_s[i, mine, :] for i in range(lat // 128)], axis=1)
                qr = qr_s[mine, :][:, 0:rope]
                ck = jnp.concatenate([ckv_b[slot, c, j] for c in range(lat // 128)], axis=1)
                s = (dot_nt(ql.astype(BF16), ck) + dot(qr.astype(BF16), kpe_b[slot, j])) * scale
                s = jnp.where(position < len_ref[b], s, -jnp.inf)
                cn_b = cn_s[pl.ds(b, 1), :]
                kn_b = kn_s[pl.ds(b, 1), :]
                s_new = (jnp.sum(ql * cn_b, axis=1, keepdims=True) + jnp.sum(qr * kn_b, axis=1, keepdims=True)) * scale
                m = jnp.maximum(jnp.max(s, axis=1, keepdims=True), s_new)
                e = jnp.exp(s - m)
                e_new = jnp.exp(s_new - m)
                total = jnp.sum(e, axis=1, keepdims=True) + e_new
                acc = dot(e.astype(BF16), ck) + e_new.astype(BF16).astype(F32) * cn_b
                out = (acc / total).astype(BF16).astype(F32)
                for i in range(lat // 128):
                    ql_s[i, mine, :] = out[:, i * 128:(i + 1) * 128]

        @pl.when(step + slots < steps)
        def _():
            for c in ccopy(step + slots, slot):
                c.start()

        return carry

    lax.fori_loop(0, steps, attend, 0)

    with jax.named_scope("w_uv"):
        c_uv.wait()
    quad_lane = lax.broadcasted_iota(jnp.int32, (rows, 4 * nope), 1) // nope

    def head_out(g, carry):
        lat_out = jnp.concatenate([
            jnp.concatenate([ql_s.at[i][pl.ds(g * 4 + k, rows, stride=heads), :] for i in range(lat // 128)], axis=1)
            for k in range(4)], axis=0).astype(BF16)
        full = dot_nt(lat_out, wide(wuv, pl.ds(pl.multiple_of(g * 4 * nope, 256), 4 * nope)))
        o = full[0:rows]
        for j in range(1, 4):
            o = jnp.where(quad_lane == j, full[j * rows:(j + 1) * rows], o)
        o_s[g] = o.astype(BF16)
        return carry

    with jax.named_scope("headout"):
        lax.fori_loop(0, heads // 4, head_out, 0)

    with jax.named_scope("w_out"):
        c_out.wait()
    with jax.named_scope("outproj"):
        o_all = jnp.concatenate([o_s[g] for g in range(heads // 4)], axis=1)
        for n in range(wout.shape[0] // 2):
            at = slice(n * 256, (n + 1) * 256)
            w = jnp.concatenate([wout[2 * n], wout[2 * n + 1]], axis=1)
            r_ref[:, at] = (x_ref[:, at].astype(F32) + dot(o_all, w)).astype(BF16)
    u = normed(r_ref[...].astype(F32), g2_ref[...]).astype(BF16)
    for c in range(u_ref.shape[0]):
        u_ref[c] = u[:, c * 128:(c + 1) * 128]


def slabs(w):
    return pltpu.VMEM((w.shape[1] // 128, w.shape[0], 128), BF16)


def attention_rows(hidden, ckv_cache, kpe_cache, cache_len, rope_cos, rope_sin, norm_attn, w_dq, norm_q, w_uq, w_dkv, norm_kv, w_uk, w_uv, w_out, norm_mlp):
    rows, width = hidden.shape
    q_lora, heads, qk = w_uq.shape
    lat, _, nope = w_uk.shape
    rope = kpe_cache.shape[2]
    seq = ckv_cache.shape[1]
    per, slots = 4, 3
    dims = (heads, nope, rope, qk, lat, per, slots)
    vm = pl.BlockSpec(memory_space=pltpu.VMEM)
    hbm = pl.BlockSpec(memory_space=pl.ANY)
    wdkv_t = w_dkv.T
    wuq_t = w_uq.transpose(1, 2, 0).reshape(heads * qk, q_lora)
    wuk_t = w_uk.transpose(1, 2, 0).reshape(heads * nope, lat)
    wuv_t = w_uv.transpose(1, 2, 0).reshape(heads * nope, lat)
    wout2 = w_out.reshape(heads * nope, width)
    r, u, cn, kn_t = pl.pallas_call(
        functools.partial(attention_kernel, dims),
        out_shape=(jax.ShapeDtypeStruct((rows, width), BF16), jax.ShapeDtypeStruct((width // 128, rows, 128), BF16),
                   jax.ShapeDtypeStruct((rows, lat), BF16), jax.ShapeDtypeStruct((rope, rows), BF16)),
        in_specs=[pl.BlockSpec(memory_space=pltpu.SMEM)] + [vm] * 7 + [hbm] * 8,
        out_specs=(vm,) * 4,
        scratch_shapes=[
            pltpu.VMEM((lat // 128, heads * rows, 128), F32),
            pltpu.VMEM((heads * rows, 128), F32),
            pltpu.VMEM((rows, lat), F32),
            pltpu.VMEM((rows, rope), F32),
            pltpu.VMEM((heads // 4, rows, 4 * nope), BF16),
            pltpu.VMEM((128, 128), F32),
            slabs(w_dq),
            slabs(wdkv_t),
            slabs(wuq_t),
            slabs(wuk_t),
            slabs(wuv_t),
            slabs(wout2),
            pltpu.VMEM((slots, lat // 128, per, seq, 128), BF16),
            pltpu.VMEM((slots, per, rope, seq), BF16),
            pltpu.SemaphoreType.DMA((5 + heads * rope // 256,)),
            pltpu.SemaphoreType.DMA((slots, lat // 128 + 1)),
        ],
        compiler_params=pltpu.CompilerParams(vmem_limit_bytes=VMEM_LIMIT),
        name="attention",
    )(cache_len, hidden, norm_attn.reshape(1, -1), norm_q.reshape(1, -1), norm_kv.reshape(1, -1), norm_mlp.reshape(1, -1),
      rope_cos.T, rope_sin.T, w_dq, wdkv_t, wuq_t, wuk_t, wuv_t, wout2, ckv_cache, kpe_cache.transpose(0, 2, 1))
    return r, u, cn, kn_t.T


def mlp_kernel(n, u_ref, r_ref, wg_hbm, wu_hbm, wd_hbm, out_ref,
               ub, wg, wu, wd, wdp, ym, yp, yr, part, acc, fin, wsem, send, recv):
    me = lax.axis_index("dp")
    core = lax.rem(me, 2)
    partner = me + 1 - 2 * core
    right, left = lax.rem(me + 2, n), lax.rem(me + n - 2, n)
    slab = u_ref.shape[0]
    rows = u_ref.shape[1]
    low, high, whole = pl.ds(0, slab // 2), pl.ds(slab // 2, slab // 2), pl.ds(0, slab)

    def wcopy(src, dst, i):
        return Copies([pltpu.make_async_copy(src.at[:, pl.ds(c * 128, 128)], dst.at[c], wsem.at[i, c]) for c in range(slab)])

    def push(i, src, dst, to):
        return pltpu.make_async_remote_copy(src_ref=src, dst_ref=dst, send_sem=send.at[i], recv_sem=recv.at[i],
                                            device_id={"dp": to}, device_id_type=pl.DeviceIdType.MESH)

    c_d, c_g, c_u = wcopy(wd_hbm, wd, 0), wcopy(wg_hbm, wg, 1), wcopy(wu_hbm, wu, 2)
    c_d.start()
    c_g.start()
    c_u.start()

    with jax.named_scope("barrier"):
        barrier = pltpu.get_barrier_semaphore()
        for other in (left, right, partner):
            pl.semaphore_signal(barrier, inc=1, device_id={"dp": other}, device_id_type=pl.DeviceIdType.MESH)
        pl.semaphore_wait(barrier, 3)

    mine = [push(0, u_ref.at[low], ub.at[2, 0, low], right), push(1, u_ref.at[high], ub.at[1, 0, high], left),
            push(2, u_ref.at[high], ub.at[2, 0, high], right), push(3, u_ref.at[low], ub.at[1, 0, low], left),
            push(4, u_ref, ub.at[0, 1], partner)]
    on_right = push(5, ub.at[2, 0, low], ub.at[3, 0, low], right)
    on_left = push(6, ub.at[1, 0, high], ub.at[3, 0, high], left)
    share = {(p, h): push(7 + 2 * (p - 1) + h, ub.at[p, 0, at], ub.at[p, 1, at], partner)
             for p in (1, 2, 3) for h, at in ((0, low), (1, high))}
    give_wd = push(13, wd, wdp, partner)
    for c in mine:
        c.start()
    ub[0, 0] = u_ref[...]
    with jax.named_scope("wd_wait"):
        c_d.wait()
        give_wd.start()

    def give_y(s):
        return push(14 + s, yp.at[s], yr.at[s], partner)

    early = [push(18, part.at[1, high], fin.at[0, high], right), push(19, part.at[2, low], fin.at[1, low], left)]
    far = [push(20, part.at[3, low], acc.at[0], right), push(21, part.at[3, high], acc.at[1], left)]
    late = [push(22, part.at[1, low], fin.at[0, low], right), push(23, part.at[2, high], fin.at[1, high], left)]

    def gate_up(s):
        both = jnp.concatenate([jnp.concatenate([ub[s, 0, c], ub[s, 1, c]], axis=0) for c in range(slab)], axis=1)
        gate = dot_nt(both, wide(wg))
        up = dot_nt(both, wide(wu))
        y = (gate / (1.0 + jnp.exp(-gate)) * up).astype(BF16)
        ym[s] = y[:rows]
        yp[s] = y[rows:]

    def down(s):
        y_mine, y_other = ym[s], yr[s]
        for c in range(0, slab, 2):
            at = slice(c, c + 2)
            p = (dot(y_mine, jnp.concatenate([wd[c], wd[c + 1]], axis=1))
                 + dot(y_other, jnp.concatenate([wdp[c], wdp[c + 1]], axis=1)))
            part[s, c] = p[:, :128]
            part[s, c + 1] = p[:, 128:]

    def step(s, carry):
        with jax.named_scope("u_wait"):
            @pl.when(s == 0)
            def _():
                c_g.wait()
                c_u.wait()
                mine[4].wait_recv()

            @pl.when(s == 1)
            def _():
                share[1, 0].wait_recv()
                share[1, 1].wait_recv()

            @pl.when(s == 2)
            def _():
                share[2, 0].wait_recv()
                share[2, 1].wait_recv()

            @pl.when(s == 3)
            def _():
                share[3, 0].wait_recv()
                share[3, 1].wait_recv()

        @pl.when(s < 4)
        def _():
            with jax.named_scope("gateup"):
                gate_up(s)
                give_y(s).start()

        @pl.when(s == 0)
        def _():
            with jax.named_scope("fwd0"):
                mine[1].wait_recv()
                on_left.start()
                mine[0].wait_recv()
                on_right.start()
                share[1, 1].start()
                share[2, 0].start()
                mine[3].wait_recv()
                share[1, 0].start()
                mine[2].wait_recv()
                share[2, 1].start()
                give_wd.wait_recv()

        @pl.when(s == 1)
        def _():
            with jax.named_scope("fwd1"):
                on_right.wait_recv()
                share[3, 0].start()
                on_left.wait_recv()
                share[3, 1].start()

        @pl.when(s > 0)
        def _():
            with jax.named_scope("y_wait"):
                give_y(s - 1).wait_recv()
            with jax.named_scope("down"):
                down(s - 1)

        @pl.when(s == 2)
        def _():
            early[0].start()

        @pl.when(s == 3)
        def _():
            early[1].start()

        @pl.when(s == 4)
        def _():
            far[0].start()
            far[1].start()

        return carry

    lax.fori_loop(0, 5, step, 0)

    with jax.named_scope("base"):
        for c in range(slab):
            part[0, c] = part[0, c] + r_ref[:, c * 128:(c + 1) * 128].astype(F32)
    with jax.named_scope("far0"):
        far[0].wait_recv()
    part[1, low] = part[1, low] + acc[0]
    late[0].start()
    with jax.named_scope("far1"):
        far[1].wait_recv()
    part[2, high] = part[2, high] + acc[1]
    late[1].start()
    with jax.named_scope("early"):
        early[0].wait_recv()
        early[1].wait_recv()
    with jax.named_scope("sendwait"):
        for c in mine + [on_right, on_left, give_wd] + list(share.values()) + [give_y(s) for s in range(4)] + early + far:
            c.wait_send()
    with jax.named_scope("final"):
        for h, c in ((0, late[0]), (1, late[1])):
            c.wait_recv()
            base = h * slab // 2
            for i in range(base, base + slab // 2):
                out_ref[:, i * 128:(i + 1) * 128] = (part[0, i] + fin[0, i] + fin[1, i]).astype(BF16)
        for c in late:
            c.wait_send()


def mlp_rows(n, u, r, w_gate, w_up, w_down):
    slab, rows, _ = u.shape
    hidden = w_down.shape[0]
    vm = pl.BlockSpec(memory_space=pltpu.VMEM)
    hbm = pl.BlockSpec(memory_space=pl.ANY)
    weight = pltpu.VMEM((slab, hidden, 128), BF16)
    return pl.pallas_call(
        functools.partial(mlp_kernel, n),
        out_shape=jax.ShapeDtypeStruct(r.shape, BF16),
        in_specs=[vm, vm, hbm, hbm, hbm],
        out_specs=vm,
        scratch_shapes=[
            pltpu.VMEM((4, 2, slab, rows, 128), BF16),
            weight, weight, weight, weight,
            pltpu.VMEM((4, rows, hidden), BF16),
            pltpu.VMEM((4, rows, hidden), BF16),
            pltpu.VMEM((4, rows, hidden), BF16),
            pltpu.VMEM((4, slab, rows, 128), F32),
            pltpu.VMEM((2, slab // 2, rows, 128), F32),
            pltpu.VMEM((2, slab, rows, 128), F32),
            pltpu.SemaphoreType.DMA((3, slab)),
            pltpu.SemaphoreType.DMA((24,)),
            pltpu.SemaphoreType.DMA((24,)),
        ],
        compiler_params=pltpu.CompilerParams(vmem_limit_bytes=VMEM_LIMIT, collective_id=0, has_side_effects=True),
        name="mlp",
    )(u, r, w_gate.T, w_up.T, w_down)


def solution(mesh):
    n = mesh.shape['dp']
    row_spec = P(('rep', 'dp'), None)
    cube_spec = P(('rep', 'dp'), None, None)
    full_spec = P()
    in_specs = (row_spec, cube_spec, cube_spec, P(('rep', 'dp')), row_spec, row_spec,
                full_spec, full_spec, full_spec, full_spec, full_spec, full_spec, full_spec, full_spec, full_spec, full_spec,
                P(None, 'dp'), P(None, 'dp'), P('dp', None))

    def local_step(hidden, ckv_cache, kpe_cache, cache_len, rope_cos, rope_sin, norm_attn, w_dq, norm_q, w_uq, w_dkv, norm_kv, w_uk, w_uv, w_out, norm_mlp, w_gate, w_up, w_down):
        residual, mlp_in, ckv_new, kpe_new = attention_rows(
            hidden, ckv_cache, kpe_cache, cache_len, rope_cos, rope_sin, norm_attn, w_dq, norm_q, w_uq, w_dkv, norm_kv, w_uk, w_uv, w_out, norm_mlp)
        out_hidden = mlp_rows(n, mlp_in, residual, w_gate, w_up, w_down)
        return out_hidden, ckv_new, kpe_new

    return jax.shard_map(local_step, mesh=mesh, in_specs=in_specs, out_specs=(row_spec, row_spec, row_spec), check_vma=False)
```
